32 devices in a mesh: trial: 4 (over y, x), dp: 4 (over z), tp: 2 (over core).
Axes of the slice: x: 2, y: 2, z: 4, core: 2. Of those that a mesh axis runs over, the one named last changes fastest.
Arguments:
- slope_query: float32 [16, 768, 768], P(('trial', 'dp'), None, 'tp'), parts along dimension 0, may hold values from -4 to 4
- slope_key: float32 [16, 768, 768], P(('trial', 'dp'), None, 'tp'), parts along dimension 0, may hold values from -4 to 4
- slope_value: float32 [16, 768, 768], P(('trial', 'dp'), None, 'tp'), parts along dimension 0, may hold values from -4 to 4
- slope_mixed: float32 [16, 768, 768], P(('trial', 'dp'), 'tp'), parts along dimension 0, may hold values from -4 to 4
- slope_norm: float32 [16, 768], P(('trial', 'dp')), parts along dimension 0, may hold values from -8 to 8
- slope_bias: float32 [16, 768], P(('trial', 'dp')), parts along dimension 0, may hold values from -8 to 8
- param_query: float32 [3072, 768], P(('trial', 'dp'), 'tp'), parts along dimension 0, may hold values from -0.3125 to 0.3125
- param_key: float32 [3072, 768], P(('trial', 'dp'), 'tp'), parts along dimension 0, may hold values from -0.3125 to 0.3125
- param_value: float32 [3072, 768], P(('trial', 'dp'), 'tp'), parts along dimension 0, may hold values from -0.3125 to 0.3125
- param_mixed: float32 [3072, 768], P(('trial', 'tp'), 'dp'), parts along dimension 0, may hold values from -0.3125 to 0.3125
- param_norm: float32 [3072], P(('trial', 'dp')), parts along dimension 0, may hold values from 0.25 to 1.75
- param_bias: float32 [3072], P(('trial', 'dp')), parts along dimension 0, may hold values from -3 to 3
- state_query: float32 [3072, 768], P(('trial', 'dp'), 'tp'), parts along dimension 0, may hold values from 0.00026041668 to 0.0026041667
- state_key: float32 [3072, 768], P(('trial', 'dp'), 'tp'), parts along dimension 0, may hold values from 0.00026041668 to 0.0026041667
- state_value: float32 [3072, 768], P(('trial', 'dp'), 'tp'), parts along dimension 0, may hold values from 0.00026041668 to 0.0026041667
- state_mixed: float32 [3072, 768], P(('trial', 'tp'), 'dp'), parts along dimension 0, may hold values from 0.00026041668 to 0.0026041667
- state_norm: float32 [3072], P(('trial', 'dp')), parts along dimension 0, may hold values from 0.05 to 0.8
- state_bias: float32 [3072], P(('trial', 'dp')), parts along dimension 0, may hold values from 0.05 to 0.8
Outputs:
- half_query: bfloat16 [3072, 768], P('trial', 'tp'), parts along dimension 0
- half_key: bfloat16 [3072, 768], P('trial', 'tp'), parts along dimension 0
- half_value: bfloat16 [3072, 768], P('trial', 'tp'), parts along dimension 0
- half_mixed: bfloat16 [3072, 768], P(('trial', 'tp')), parts along dimension 0
- half_norm: bfloat16 [3072], P('trial'), parts along dimension 0
- half_bias: bfloat16 [3072], P('trial'), parts along dimension 0
- next_query: float32 [3072, 768], P(('trial', 'dp'), 'tp'), parts along dimension 0
- next_key: float32 [3072, 768], P(('trial', 'dp'), 'tp'), parts along dimension 0
- next_value: float32 [3072, 768], P(('trial', 'dp'), 'tp'), parts along dimension 0
- next_mixed: float32 [3072, 768], P(('trial', 'tp'), 'dp'), parts along dimension 0
- next_norm: float32 [3072], P(('trial', 'dp')), parts along dimension 0
- next_bias: float32 [3072], P(('trial', 'dp')), parts along dimension 0
- state_new_query: float32 [3072, 768], P(('trial', 'dp'), 'tp'), parts along dimension 0
- state_new_key: float32 [3072, 768], P(('trial', 'dp'), 'tp'), parts along dimension 0
- state_new_value: float32 [3072, 768], P(('trial', 'dp'), 'tp'), parts along dimension 0
- state_new_mixed: float32 [3072, 768], P(('trial', 'tp'), 'dp'), parts along dimension 0
- state_new_norm: float32 [3072], P(('trial', 'dp')), parts along dimension 0
- state_new_bias: float32 [3072], P(('trial', 'dp')), parts along dimension 0
The draws below stay inside these ranges and needn't reach their ends.
There are 4 independent parts, one for each index of `trial`. The reference program is written for one: setup_inputs(seed, part) draws one part's arguments, and reference() takes and returns one part's arrays. A program takes and returns all parts, laid end to end along the dimension named above; each array names one. Nothing has to cross between parts.
All inputs are finite; a program needn't handle non-finite values.
Results may differ from the reference program's by a relative error of at most 0.001.
Values may be sent and summed in bfloat16 or wider, within the bound.
A program may use at most 64 MiB of HBM per device.

```python
import jax
import jax.numpy as jnp
from jax import lax

WIDTH = 768
ATTN = 768
REPLICAS = 4


def with_spikes(entries, rng, source, target, parts, factor):
    owner, partner = [(jnp.arange(entries.shape[position]) // (entries.shape[position] // parts)).reshape([-1 if axis == position else 1 for axis in range(entries.ndim)]) for position in (source, target)]
    chosen = jax.random.permutation(rng, parts)[partner]
    strong = (owner == chosen) | (owner == (partner + parts // 2) % parts)
    return jnp.where(strong, factor * entries, entries)


def steps_of(stream_key, shape, split, low, top_value):
    gain = 1.0
    for axis_at, blocks in split:
        steps = jax.random.uniform(jax.random.fold_in(jax.random.fold_in(stream_key, 6), axis_at), (blocks,), jnp.float32, low / len(split), top_value / len(split))
        gain = gain * jnp.repeat(jnp.exp(steps), shape[axis_at] // blocks).reshape((-1,) + (1,) * (len(shape) - 1 - axis_at))
    return gain


def gaussian(rng, extent, scale, most, cuts=(), dtype=jnp.bfloat16):
    factor_of = steps_of(rng, extent, cuts, -0.22, 0.18) if cuts else 1.0
    result = jax.random.normal(rng, extent, jnp.float32) * scale * factor_of
    return jnp.minimum(jnp.maximum(result, -most), most).astype(dtype)


def gaussian_with(key, dims, width, most, shards, heavy, held_as=jnp.bfloat16):
    values = width * jax.random.normal(key, dims, jnp.float32)
    if shards:
        values = values * steps_of(key, dims, shards, -0.22, 0.18)
    return jnp.clip(with_spikes(values, jax.random.fold_in(key, 3), *heavy), -most, most).astype(held_as)


def setup_inputs(seed: int = 0, part: int = 0) -> dict:
    streams_of = jax.random.split(jax.random.key(seed), 19)
    part_splits = jax.random.split(jax.random.fold_in(streams_of[18], part), 19)
    return {
        "slope_query": gaussian_with(part_splits[0], (REPLICAS, WIDTH, ATTN), 0.5, 4.0, ((0, 4), (2, 2)), (0, 1, 4, 2.0), jnp.float32),
        "slope_key": gaussian_with(part_splits[1], (REPLICAS, WIDTH, ATTN), 0.5, 4.0, ((0, 4), (2, 2)), (0, 1, 4, 2.0), jnp.float32),
        "slope_value": gaussian_with(part_splits[2], (REPLICAS, WIDTH, ATTN), 0.5, 4.0, ((0, 4), (2, 2)), (0, 1, 4, 2.0), jnp.float32),
        "slope_mixed": gaussian_with(part_splits[3], (REPLICAS, ATTN, WIDTH), 0.5, 4.0, ((0, 4), (1, 2)), (0, 2, 4, 2.0), jnp.float32),
        "slope_norm": gaussian_with(part_splits[4], (REPLICAS, WIDTH), 1.0, 8.0, ((0, 4),), (0, 1, 4, 2.0), jnp.float32),
        "slope_bias": gaussian_with(part_splits[5], (REPLICAS, WIDTH), 1.0, 8.0, ((0, 4),), (0, 1, 4, 2.0), jnp.float32),
        "param_query": gaussian_with(part_splits[6], (WIDTH, ATTN), WIDTH ** -0.5, 0.3125, ((0, 4), (1, 2)), (1, 0, 4, 2.0), jnp.float32),
        "param_key": gaussian_with(part_splits[7], (WIDTH, ATTN), WIDTH ** -0.5, 0.3125, ((0, 4), (1, 2)), (1, 0, 4, 2.0), jnp.float32),
        "param_value": gaussian_with(part_splits[8], (WIDTH, ATTN), WIDTH ** -0.5, 0.3125, ((0, 4), (1, 2)), (1, 0, 4, 2.0), jnp.float32),
        "param_mixed": gaussian_with(part_splits[9], (ATTN, WIDTH), ATTN ** -0.5, 0.3125, ((0, 2), (1, 4)), (0, 1, 4, 2.0), jnp.float32),
        "param_norm": jnp.clip(1.0 + 0.15 * jax.random.normal(part_splits[10], (WIDTH,), jnp.float32), 0.25, 1.75),
        "param_bias": gaussian(part_splits[11], (WIDTH,), 0.5, 3.0, ((0, 4),), jnp.float32),
        "state_query": jnp.clip(0.00026041668 + 0.00234375 * jax.random.uniform(part_splits[12], (WIDTH, ATTN), jnp.float32) ** steps_of(part_splits[12], (WIDTH, ATTN), ((0, 4), (1, 2)), -0.2, 0.2), 0.00026041668, 0.0026041667),
        "state_key": jnp.clip(0.00026041668 + 0.00234375 * jax.random.uniform(part_splits[13], (WIDTH, ATTN), jnp.float32) ** steps_of(part_splits[13], (WIDTH, ATTN), ((0, 4), (1, 2)), -0.2, 0.2), 0.00026041668, 0.0026041667),
        "state_value": jnp.clip(0.00026041668 + 0.00234375 * jax.random.uniform(part_splits[14], (WIDTH, ATTN), jnp.float32) ** steps_of(part_splits[14], (WIDTH, ATTN), ((0, 4), (1, 2)), -0.2, 0.2), 0.00026041668, 0.0026041667),
        "state_mixed": jnp.clip(0.00026041668 + 0.00234375 * jax.random.uniform(part_splits[15], (ATTN, WIDTH), jnp.float32) ** steps_of(part_splits[15], (ATTN, WIDTH), ((0, 2), (1, 4)), -0.2, 0.2), 0.00026041668, 0.0026041667),
        "state_norm": jnp.clip(0.05 + 0.75 * jax.random.uniform(part_splits[16], (WIDTH,), jnp.float32) ** steps_of(part_splits[16], (WIDTH,), ((0, 4),), -0.2, 0.2), 0.05, 0.8),
        "state_bias": jnp.clip(0.05 + 0.75 * jax.random.uniform(part_splits[17], (WIDTH,), jnp.float32) ** steps_of(part_splits[17], (WIDTH,), ((0, 4),), -0.2, 0.2), 0.05, 0.8),
    }


learn_rate = 0.02
hold_rate = 0.8

def reference(slope_query, slope_key, slope_value, slope_mixed, slope_norm, slope_bias, param_query, param_key, param_value, param_mixed, param_norm, param_bias, state_query, state_key, state_value, state_mixed, state_norm, state_bias):
    mean_query = lax.optimization_barrier(jnp.sum(slope_query.astype(jnp.float32), axis=0)) * REPLICAS ** (-0.5)
    mean_key = lax.optimization_barrier(jnp.sum(slope_key.astype(jnp.float32), axis=0)) * REPLICAS ** (-0.5)
    mean_value = lax.optimization_barrier(jnp.sum(slope_value.astype(jnp.float32), axis=0)) * REPLICAS ** (-0.5)
    mean_mixed = lax.optimization_barrier(jnp.sum(slope_mixed.astype(jnp.float32), axis=0)) * REPLICAS ** (-0.5)
    mean_norm = lax.optimization_barrier(jnp.sum(slope_norm.astype(jnp.float32), axis=0)) * REPLICAS ** (-0.5)
    mean_bias = lax.optimization_barrier(jnp.sum(slope_bias.astype(jnp.float32), axis=0)) * REPLICAS ** (-0.5)
    ratio_query = jnp.sqrt(lax.optimization_barrier(jnp.sum(param_query * param_query, axis=1, keepdims=True))) * lax.rsqrt(lax.optimization_barrier(jnp.sum(mean_query * mean_query, axis=1, keepdims=True)) + 1e-06)
    mean_query = mean_query * ratio_query
    ratio_key = jnp.sqrt(lax.optimization_barrier(jnp.sum(param_key * param_key, axis=1, keepdims=True))) * lax.rsqrt(lax.optimization_barrier(jnp.sum(mean_key * mean_key, axis=1, keepdims=True)) + 1e-06)
    mean_key = mean_key * ratio_key
    ratio_value = jnp.sqrt(lax.optimization_barrier(jnp.sum(param_value * param_value, axis=1, keepdims=True))) * lax.rsqrt(lax.optimization_barrier(jnp.sum(mean_value * mean_value, axis=1, keepdims=True)) + 1e-06)
    mean_value = mean_value * ratio_value
    ratio_mixed = jnp.sqrt(lax.optimization_barrier(jnp.sum(param_mixed * param_mixed, axis=0, keepdims=True))) * lax.rsqrt(lax.optimization_barrier(jnp.sum(mean_mixed * mean_mixed, axis=0, keepdims=True)) + 1e-06)
    mean_mixed = mean_mixed * ratio_mixed
    state_new_query = hold_rate * state_query + (1.0 - hold_rate) * mean_query * mean_query
    next_query = param_query - learn_rate * mean_query * lax.rsqrt(state_new_query + 1e-06)
    state_new_key = hold_rate * state_key + (1.0 - hold_rate) * mean_key * mean_key
    next_key = param_key - learn_rate * mean_key * lax.rsqrt(state_new_key + 1e-06)
    state_new_value = hold_rate * state_value + (1.0 - hold_rate) * mean_value * mean_value
    next_value = param_value - learn_rate * mean_value * lax.rsqrt(state_new_value + 1e-06)
    state_new_mixed = hold_rate * state_mixed + (1.0 - hold_rate) * mean_mixed * mean_mixed
    next_mixed = param_mixed - learn_rate * mean_mixed * lax.rsqrt(state_new_mixed + 1e-06)
    state_new_norm = hold_rate * state_norm + (1.0 - hold_rate) * mean_norm * mean_norm
    next_norm = param_norm - learn_rate * mean_norm * lax.rsqrt(state_new_norm + 1e-06)
    state_new_bias = hold_rate * state_bias + (1.0 - hold_rate) * mean_bias * mean_bias
    next_bias = param_bias - learn_rate * mean_bias * lax.rsqrt(state_new_bias + 1e-06)
    half_query = next_query.astype(jnp.bfloat16)
    half_key = next_key.astype(jnp.bfloat16)
    half_value = next_value.astype(jnp.bfloat16)
    half_mixed = next_mixed.astype(jnp.bfloat16)
    half_norm = next_norm.astype(jnp.bfloat16)
    half_bias = next_bias.astype(jnp.bfloat16)
    return (half_query, half_key, half_value, half_mixed, half_norm, half_bias, next_query, next_key, next_value, next_mixed, next_norm, next_bias, state_new_query, state_new_key, state_new_value, state_new_mixed, state_new_norm, state_new_bias)
```

```python
import functools

import jax
import jax.numpy as jnp
from jax import lax
from jax.experimental import pallas as pl
from jax.experimental.pallas import tpu as pltpu
from jax.sharding import PartitionSpec as P

learn_rate = 0.02
hold_rate = 0.8


def shards(
    slope_query,
    slope_key,
    slope_value,
    slope_mixed,
    slope_norm,
    slope_bias,
    param_query,
    param_key,
    param_value,
    param_mixed,
    param_norm,
    param_bias,
    state_query,
    state_key,
    state_value,
    state_mixed,
    state_norm,
    state_bias,
):
    mean_query, mean_key, mean_value, mean_mixed = (
        lax.psum_scatter(slope_query[0], "dp", scatter_dimension=0, tiled=True),
        lax.psum_scatter(slope_key[0], "dp", scatter_dimension=0, tiled=True),
        lax.psum_scatter(slope_value[0], "dp", scatter_dimension=0, tiled=True),
        lax.psum_scatter(slope_mixed[0], "dp", scatter_dimension=1, tiled=True),
    )
    whole_norm, whole_bias = lax.psum((slope_norm[0], slope_bias[0]), "dp")
    place = lax.axis_index("dp")
    mean_norm = lax.dynamic_slice_in_dim(
        whole_norm, place * param_norm.shape[0], param_norm.shape[0]
    )
    mean_bias = lax.dynamic_slice_in_dim(
        whole_bias, place * param_bias.shape[0], param_bias.shape[0]
    )
    mean_rate = lax.axis_size("dp") ** (-0.5)
    mean_query = mean_query * mean_rate
    mean_key = mean_key * mean_rate
    mean_value = mean_value * mean_rate
    mean_mixed = mean_mixed * mean_rate
    mean_norm = mean_norm * mean_rate
    mean_bias = mean_bias * mean_rate
    (
        own_query,
        own_key,
        own_value,
        own_mixed,
        slope_query_norm,
        slope_key_norm,
        slope_value_norm,
        slope_mixed_norm,
    ) = lax.psum(
        (
            jnp.sum(param_query * param_query, axis=1, keepdims=True),
            jnp.sum(param_key * param_key, axis=1, keepdims=True),
            jnp.sum(param_value * param_value, axis=1, keepdims=True),
            jnp.sum(param_mixed * param_mixed, axis=0, keepdims=True),
            jnp.sum(mean_query * mean_query, axis=1, keepdims=True),
            jnp.sum(mean_key * mean_key, axis=1, keepdims=True),
            jnp.sum(mean_value * mean_value, axis=1, keepdims=True),
            jnp.sum(mean_mixed * mean_mixed, axis=0, keepdims=True),
        ),
        "tp",
    )
    mean_query = mean_query * (jnp.sqrt(own_query) * lax.rsqrt(slope_query_norm + 1e-06))
    mean_key = mean_key * (jnp.sqrt(own_key) * lax.rsqrt(slope_key_norm + 1e-06))
    mean_value = mean_value * (jnp.sqrt(own_value) * lax.rsqrt(slope_value_norm + 1e-06))
    mean_mixed = mean_mixed * (jnp.sqrt(own_mixed) * lax.rsqrt(slope_mixed_norm + 1e-06))
    state_new_query = hold_rate * state_query + (1.0 - hold_rate) * mean_query * mean_query
    next_query = param_query - learn_rate * mean_query * lax.rsqrt(state_new_query + 1e-06)
    state_new_key = hold_rate * state_key + (1.0 - hold_rate) * mean_key * mean_key
    next_key = param_key - learn_rate * mean_key * lax.rsqrt(state_new_key + 1e-06)
    state_new_value = hold_rate * state_value + (1.0 - hold_rate) * mean_value * mean_value
    next_value = param_value - learn_rate * mean_value * lax.rsqrt(state_new_value + 1e-06)
    state_new_mixed = hold_rate * state_mixed + (1.0 - hold_rate) * mean_mixed * mean_mixed
    next_mixed = param_mixed - learn_rate * mean_mixed * lax.rsqrt(state_new_mixed + 1e-06)
    state_new_norm = hold_rate * state_norm + (1.0 - hold_rate) * mean_norm * mean_norm
    next_norm = param_norm - learn_rate * mean_norm * lax.rsqrt(state_new_norm + 1e-06)
    state_new_bias = hold_rate * state_bias + (1.0 - hold_rate) * mean_bias * mean_bias
    next_bias = param_bias - learn_rate * mean_bias * lax.rsqrt(state_new_bias + 1e-06)
    half_query, half_key, half_value, half_mixed, half_norm, half_bias = (
        lax.all_gather(next_query.astype(jnp.bfloat16), "dp", axis=0, tiled=True),
        lax.all_gather(next_key.astype(jnp.bfloat16), "dp", axis=0, tiled=True),
        lax.all_gather(next_value.astype(jnp.bfloat16), "dp", axis=0, tiled=True),
        lax.all_gather(next_mixed.astype(jnp.bfloat16), "dp", axis=1, tiled=True),
        lax.all_gather(next_norm.astype(jnp.bfloat16), "dp", axis=0, tiled=True),
        lax.all_gather(next_bias.astype(jnp.bfloat16), "dp", axis=0, tiled=True),
    )
    return (
        half_query,
        half_key,
        half_value,
        half_mixed,
        half_norm,
        half_bias,
        next_query,
        next_key,
        next_value,
        next_mixed,
        next_norm,
        next_bias,
        state_new_query,
        state_new_key,
        state_new_value,
        state_new_mixed,
        state_new_norm,
        state_new_bias,
    )


MESH = pl.DeviceIdType.MESH
HALVES = 2
GAIN = 1024.0
ORDER = (0, 3, 1, 2)


def plan_of(mesh):
    n, pair = mesh.shape["dp"], mesh.shape["tp"]
    return n if pair == 2 and n == 4 else None


def encode(x):
    t = x * GAIN
    t = t * t
    t = t * t
    t = t * t
    return jnp.where(x < 0, -t, t).astype(jnp.bfloat16)


def decode(y):
    y = y.astype(jnp.float32)
    fourth = lax.rsqrt(lax.rsqrt(jnp.abs(y)))
    root = fourth * lax.rsqrt(jnp.maximum(fourth, 1e-30)) * (1.0 / GAIN)
    return jnp.where(y < 0, -root, root)


def update(param, state, mean):
    state_new = hold_rate * state + (1.0 - hold_rate) * mean * mean
    return state_new, param - learn_rate * mean * lax.rsqrt(state_new + 1e-06)


def kernel(n, *refs):
    (sq, sk, sv, sm, sn, sb, pq, pk, pv, pm, pn, pb, tq, tk, tv, tm, tn, tb) = refs[:18]
    (hq, hk, hv, hm, hn, hb, xq, xk, xv, xm, xn, xb, nq, nk, nv, nm, nn, nb) = refs[18:36]
    (X, XM, S, RL, RR, G, P_, T_, PM, TM, NX, NS, TOT, ES, ER, HM, VB, VR, NV,
     load_sem, mix_sem, par_sem, rs_send, rl_sem, rr_sem, ag_send, ag_send2, ag_recv,
     e_send, e_recv, v_send, v_recv, out_sem, half_sem) = refs[36:]
    C, _, B, W = X.shape
    H = HALVES
    own = B * H
    mixc = H * ORDER.index(3)
    me = lax.axis_index("dp")
    core = lax.axis_index("tp")
    rate = float(n) ** (-0.5)
    slopes = (sq, sk, sv)
    order = [n - 1, 0] + [j for j in range(n - 2, 0, -1)]

    loads = [None] * C
    for at, m in enumerate(ORDER):
        if m < 3:
            for h in range(H):
                c = at * H + h
                loads[c] = pltpu.make_async_copy(slopes[m].at[:, h], X.at[c], load_sem.at[c])
                loads[c].start()
        else:
            mix = pltpu.make_async_copy(sm, XM, mix_sem)
            mix.start()
    pars = []
    for at, m in enumerate(ORDER):
        for k, (srcs, dst, odd) in enumerate((((pq, pk, pv, pm), P_, PM), ((tq, tk, tv, tm), T_, TM))):
            d = odd if m == 3 else dst.at[pl.ds(at * H, H)]
            cp = pltpu.make_async_copy(srcs[m], d, par_sem.at[k, m])
            cp.start()
            pars.append(cp)

    barrier = pltpu.get_barrier_semaphore()
    for d in range(1, n):
        pl.semaphore_signal(barrier, inc=1, device_id={"dp": lax.rem(me + d, n)}, device_id_type=MESH)
    pl.semaphore_signal(barrier, inc=1, device_id={"tp": 1 - core}, device_id_type=MESH)

    part = sn.shape[1] // n
    for j in range(n):
        VB[j : j + 1, :part] = sn[:, j * part : (j + 1) * part]
        VB[n + j : n + j + 1, :part] = sb[:, j * part : (j + 1) * part]
    for k, r in enumerate((pn, pb, tn, tb)):
        VB[2 * n + k : 2 * n + k + 1, :part] = r[...]
    pl.semaphore_wait(barrier, n)

    def hop(src, dst, ss, rs, to):
        return pltpu.make_async_remote_copy(
            src_ref=src, dst_ref=dst, send_sem=ss, recv_sem=rs, device_id={"dp": to}, device_id_type=MESH
        )

    right, left = jnp.minimum(me + 1, n - 1), jnp.maximum(me - 1, 0)

    def rs_right(c, j):
        return hop(S.at[c, j], RL.at[c, j], rs_send.at[c, j], rl_sem.at[c, j], right)

    def rs_left(c, j):
        return hop(S.at[c, j], RR.at[c, j], rs_send.at[c, j], rr_sem.at[c, j], left)

    def ag_right(c, j):
        return hop(G.at[c, j], G.at[c, j], ag_send.at[c, j], ag_recv.at[c, j], right)

    def ag_left(c, j):
        return hop(G.at[c, j], G.at[c, j], ag_send.at[c, j], ag_recv.at[c, j], left)

    def ag_left_own(c):
        return hop(G.at[c, me], G.at[c, me], ag_send2.at[c], ag_recv.at[c, me], left)

    def vec(d):
        return hop(VB, VR.at[n - d], v_send.at[d], v_recv.at[n - d], lax.rem(me + d, n))

    def pair(c):
        return pltpu.make_async_remote_copy(
            src_ref=ES.at[c], dst_ref=ER.at[c], send_sem=e_send.at[c], recv_sem=e_recv.at[c],
            device_id={"tp": 1 - core}, device_id_type=MESH,
        )

    def rs(c):
        for j in order:
            for go, first, wait, land, send in (
                (me < j, me == 0, rs_right, RL, rs_right),
                (me > j, me == n - 1, rs_left, RR, rs_left),
            ):
                @pl.when(go)
                def _(j=j, first=first, wait=wait, land=land, send=send):
                    @pl.when(first)
                    def _():
                        S[c, j] = encode(X[c, j])

                    @pl.when(jnp.logical_not(first))
                    def _():
                        wait(c, j).wait_recv()
                        S[c, j] = encode(decode(land[c, j]) + X[c, j])

                    send(c, j).start()

    def gather_sum(c):
        TOT[c] = X[c, me]

        @pl.when(me > 0)
        def _():
            rs_right(c, me).wait_recv()
            TOT[c] = TOT[c] + decode(RL[c, me])

        @pl.when(me < n - 1)
        def _():
            rs_left(c, me).wait_recv()
            TOT[c] = TOT[c] + decode(RR[c, me])

        mean = TOT[c] * rate
        TOT[c] = mean
        p = P_[c]
        lane = lax.broadcasted_iota(jnp.int32, (B, 128), 1)
        ES[c] = jnp.where(
            lane < 64, jnp.sum(p * p, axis=1, keepdims=True), jnp.sum(mean * mean, axis=1, keepdims=True)
        )
        pair(c).start()

    def apply(c):
        pair(c).wait_recv()
        both = ES[c] + ER[c]
        ratio = jnp.sqrt(both[:, :1]) * lax.rsqrt(both[:, 64:65] + 1e-06)
        state_new, nxt = update(P_[c], T_[c], TOT[c] * ratio)
        G[c, me] = nxt.astype(jnp.bfloat16)
        NX[c] = nxt
        NS[c] = state_new

        @pl.when(me < n - 1)
        def _():
            ag_right(c, me).start()

        @pl.when(me > 0)
        def _():
            ag_left_own(c).start()

    def passes(j):
        return jnp.logical_or(
            jnp.logical_and(me > j, me < n - 1), jnp.logical_and(me < j, me > 0)
        )

    def take(c, j):
        ag_right(c, j).wait_recv()

        @pl.when(jnp.logical_and(me > j, me < n - 1))
        def _():
            ag_right(c, j).start()

        @pl.when(jnp.logical_and(me < j, me > 0))
        def _():
            ag_left(c, j).start()

    def mixed_in():
        mix.wait()
        for b in range(XM.shape[1] // 128):
            t = XM[:, b * 128 : b * 128 + 128].T
            for p in range(4):
                r = b * 128 + p * 32
                X[mixc + (r % own) // B, r // own, r % B : r % B + 32] = t[p * 32 : p * 32 + 32]
        for src, dst in ((PM, P_), (TM, T_)):
            t = src[...].T
            for h in range(H):
                dst[mixc + h] = t[h * B : h * B + B]

    for d in range(1, n):
        vec(d).start()
    for c in range(C):
        if loads[c] is not None and c < H:
            loads[c].wait()
    VR[0] = VB[...]
    for c in range(H):
        rs(c)
    for c in range(C):
        if loads[c] is not None and c >= H:
            loads[c].wait()
    for cp in pars:
        cp.wait()
    mixed_in()

    def step(t, carry):
        @pl.when(t < C)
        def _():
            rs(t)

        @pl.when(jnp.logical_and(t >= 1, t <= C))
        def _():
            gather_sum(t - 1)

        @pl.when(jnp.logical_and(t >= 2, t <= C + 1))
        def _():
            apply(t - 2)

        @pl.when(t >= 3)
        def _():
            for j in range(1, n - 1):
                @pl.when(passes(j))
                def _(j=j):
                    take(t - 3, j)

        return carry

    gather_sum(0)
    lax.fori_loop(H, C + 3, step, 0)

    nexts, news = (xq, xk, xv), (nq, nk, nv)
    outs = []
    for at, m in enumerate(ORDER):
        for k, (buf, dsts, odd, mo) in enumerate(((NX, nexts, PM, xm), (NS, news, TM, nm))):
            if m < 3:
                cp = pltpu.make_async_copy(buf.at[pl.ds(at * H, H)], dsts[m], out_sem.at[k, m])
            else:
                odd[...] = jnp.concatenate([buf[mixc + h] for h in range(H)], axis=0).T
                cp = pltpu.make_async_copy(odd, mo, out_sem.at[k, m])
            cp.start()
            outs.append(cp)

    for d in range(1, n):
        vec(d).wait_send()
        vec(n - d).wait_recv()
    total = VR[0, : 2 * n]
    for d in range(1, n):
        total = total + VR[d, : 2 * n]
    NV[0] = total * rate
    for d in range(n):
        at = lax.rem(me + d, n)
        for k in range(2):
            mean = NV[0, pl.ds(k * n + at, 1), :]
            state_new, nxt = update(
                VR[d, 2 * n + k : 2 * n + k + 1], VR[d, 2 * n + 2 + k : 2 * n + 3 + k], mean
            )
            NV[1, pl.ds(k * n + at, 1), :] = nxt
            if d == 0:
                (xn, xb)[k][...] = nxt[:, :part]
                (nn, nb)[k][...] = state_new[:, :part]
    for k, o in enumerate((hn, hb)):
        o[...] = jnp.concatenate(
            [NV[1, k * n + j : k * n + j + 1, :part] for j in range(n)], axis=1
        ).astype(jnp.bfloat16)

    halves = (hq, hk, hv)

    def finish(c):
        for j in range(n):
            open_ = me != j
            if 0 < j < n - 1:
                open_ = jnp.logical_and(open_, jnp.logical_not(passes(j)))

            @pl.when(open_)
            def _(j=j):
                take(c, j)

    stores = []
    for at, m in enumerate(ORDER):
        for h in range(H):
            c = at * H + h
            finish(c)
            if m < 3:
                cp = pltpu.make_async_copy(G.at[c], halves[m].at[:, h], half_sem.at[c])
                cp.start()
                stores.append(cp)
        if m == 3:
            for j in range(n // 2):
                rows = [G[at * H + h, 2 * j + i].astype(jnp.float32) for i in range(2) for h in range(H)]
                HM[:, j * 2 * own : (j + 1) * 2 * own] = jnp.concatenate(rows, axis=0).T.astype(jnp.bfloat16)
            cp = pltpu.make_async_copy(HM, hm, half_sem.at[at * H])
            cp.start()
            stores.append(cp)

    def drain(c, carry):
        for j in range(n):
            @pl.when(me != j)
            def _(j=j):
                rs_right(c, j).wait_send()

            @pl.when(jnp.logical_and(me != j, passes(j)))
            def _(j=j):
                ag_right(c, j).wait_send()

        @pl.when(me < n - 1)
        def _():
            ag_right(c, me).wait_send()

        @pl.when(me > 0)
        def _():
            ag_left_own(c).wait_send()

        pair(c).wait_send()
        return carry

    lax.fori_loop(0, C, drain, 0)
    for cp in outs + stores:
        cp.wait()


def fused(n, *args):
    slopes, params, states = list(args[:6]), list(args[6:12]), list(args[12:])
    own, width = params[0].shape
    H = HALVES
    B = own // H
    if own % (H * 32) or width % 128 or args[3].shape[1:] != (width, n * own) or args[3].shape[2] % 256:
        return shards(*args)
    C = H * 4
    for i in range(3):
        slopes[i] = slopes[i].reshape(n, H, B, width)
        params[i] = params[i].reshape(H, B, width)
        states[i] = states[i].reshape(H, B, width)
    slopes[3] = slopes[3][0]
    for group in (params, states):
        for i in (4, 5):
            group[i] = group[i].reshape(1, -1)
    any_, vmem = pl.BlockSpec(memory_space=pl.ANY), pl.BlockSpec(memory_space=pltpu.VMEM)
    f32, bf16 = jnp.float32, jnp.bfloat16
    specs = [any_] * 4 + [vmem] * 2
    S = jax.ShapeDtypeStruct
    rows = n * own
    shape = (
        [S((n, H, B, width), bf16)] * 3 + [S((width, rows), bf16)] + [S((1, rows), bf16)] * 2
        + ([S((H, B, width), f32)] * 3 + [S((width, own), f32)] + [S((1, own), f32)] * 2) * 2
    )
    wide = -(-own // 128) * 128
    dma = pltpu.SemaphoreType.DMA
    outs = pl.pallas_call(
        functools.partial(kernel, n),
        out_shape=shape,
        in_specs=specs * 3,
        out_specs=specs * 3,
        scratch_shapes=[
            pltpu.VMEM((C, n, B, width), f32),
            pltpu.VMEM((width, rows), f32),
            pltpu.VMEM((C, n, B, width), bf16),
            pltpu.VMEM((C, n, B, width), bf16),
            pltpu.VMEM((C, n, B, width), bf16),
            pltpu.VMEM((C, n, B, width), bf16),
            pltpu.VMEM((C, B, width), f32),
            pltpu.VMEM((C, B, width), f32),
            pltpu.VMEM((width, own), f32),
            pltpu.VMEM((width, own), f32),
            pltpu.VMEM((C, B, width), f32),
            pltpu.VMEM((C, B, width), f32),
            pltpu.VMEM((C, B, width), f32),
            pltpu.VMEM((C, B, 128), f32),
            pltpu.VMEM((C, B, 128), f32),
            pltpu.VMEM((width, rows), bf16),
            pltpu.VMEM((16, wide), f32),
            pltpu.VMEM((n, 16, wide), f32),
            pltpu.VMEM((2, 2 * n, wide), f32),
            dma((C,)), dma, dma((2, 4)), dma((C, n)), dma((C, n)), dma((C, n)), dma((C, n)), dma((C,)), dma((C, n)),
            dma((C,)), dma((C,)), dma((n,)), dma((n,)), dma((2, 4)), dma((C,)),
        ],
        compiler_params=pltpu.CompilerParams(
            collective_id=0, has_side_effects=True, vmem_limit_bytes=48 * 2**20
        ),
        cost_estimate=pl.CostEstimate(flops=10**7, bytes_accessed=10**7, transcendentals=0),
    )(*slopes, *params, *states)
    outs = list(outs)
    for i in range(3):
        outs[i] = outs[i].reshape(rows, width)
        for k in (6, 12):
            outs[k + i] = outs[k + i].reshape(own, width)
    for k in (4, 5, 10, 11, 16, 17):
        outs[k] = outs[k].reshape(-1)
    return tuple(outs)


def solution(mesh):
    in_specs = (
        P(("trial", "dp"), None, "tp"),
        P(("trial", "dp"), None, "tp"),
        P(("trial", "dp"), None, "tp"),
        P(("trial", "dp"), "tp", None),
        P(("trial", "dp"), None),
        P(("trial", "dp"), None),
        P(("trial", "dp"), "tp"),
        P(("trial", "dp"), "tp"),
        P(("trial", "dp"), "tp"),
        P(("trial", "tp"), "dp"),
        P(("trial", "dp")),
        P(("trial", "dp")),
        P(("trial", "dp"), "tp"),
        P(("trial", "dp"), "tp"),
        P(("trial", "dp"), "tp"),
        P(("trial", "tp"), "dp"),
        P(("trial", "dp")),
        P(("trial", "dp")),
    )
    out_specs = (
        P("trial", "tp"),
        P("trial", "tp"),
        P("trial", "tp"),
        P(("trial", "tp"), None),
        P("trial"),
        P("trial"),
        P(("trial", "dp"), "tp"),
        P(("trial", "dp"), "tp"),
        P(("trial", "dp"), "tp"),
        P(("trial", "tp"), "dp"),
        P(("trial", "dp")),
        P(("trial", "dp")),
        P(("trial", "dp"), "tp"),
        P(("trial", "dp"), "tp"),
        P(("trial", "dp"), "tp"),
        P(("trial", "tp"), "dp"),
        P(("trial", "dp")),
        P(("trial", "dp")),
    )
    plan = plan_of(mesh)
    body = shards if plan is None else functools.partial(fused, plan)
    return jax.shard_map(body, mesh=mesh, in_specs=in_specs, out_specs=out_specs, check_vma=False)
```

```python
import functools

import jax
import jax.numpy as jnp
from jax import lax
from jax.experimental import pallas as pl
from jax.experimental.pallas import tpu as pltpu
from jax.sharding import PartitionSpec as P

learn_rate = 0.02
hold_rate = 0.8


def shards(
    slope_query,
    slope_key,
    slope_value,
    slope_mixed,
    slope_norm,
    slope_bias,
    param_query,
    param_key,
    param_value,
    param_mixed,
    param_norm,
    param_bias,
    state_query,
    state_key,
    state_value,
    state_mixed,
    state_norm,
    state_bias,
):
    mean_query, mean_key, mean_value, mean_mixed = (
        lax.psum_scatter(slope_query[0], "dp", scatter_dimension=0, tiled=True),
        lax.psum_scatter(slope_key[0], "dp", scatter_dimension=0, tiled=True),
        lax.psum_scatter(slope_value[0], "dp", scatter_dimension=0, tiled=True),
        lax.psum_scatter(slope_mixed[0], "dp", scatter_dimension=1, tiled=True),
    )
    whole_norm, whole_bias = lax.psum((slope_norm[0], slope_bias[0]), "dp")
    place = lax.axis_index("dp")
    mean_norm = lax.dynamic_slice_in_dim(
        whole_norm, place * param_norm.shape[0], param_norm.shape[0]
    )
    mean_bias = lax.dynamic_slice_in_dim(
        whole_bias, place * param_bias.shape[0], param_bias.shape[0]
    )
    mean_rate = lax.axis_size("dp") ** (-0.5)
    mean_query = mean_query * mean_rate
    mean_key = mean_key * mean_rate
    mean_value = mean_value * mean_rate
    mean_mixed = mean_mixed * mean_rate
    mean_norm = mean_norm * mean_rate
    mean_bias = mean_bias * mean_rate
    (
        own_query,
        own_key,
        own_value,
        own_mixed,
        slope_query_norm,
        slope_key_norm,
        slope_value_norm,
        slope_mixed_norm,
    ) = lax.psum(
        (
            jnp.sum(param_query * param_query, axis=1, keepdims=True),
            jnp.sum(param_key * param_key, axis=1, keepdims=True),
            jnp.sum(param_value * param_value, axis=1, keepdims=True),
            jnp.sum(param_mixed * param_mixed, axis=0, keepdims=True),
            jnp.sum(mean_query * mean_query, axis=1, keepdims=True),
            jnp.sum(mean_key * mean_key, axis=1, keepdims=True),
            jnp.sum(mean_value * mean_value, axis=1, keepdims=True),
            jnp.sum(mean_mixed * mean_mixed, axis=0, keepdims=True),
        ),
        "tp",
    )
    mean_query = mean_query * (jnp.sqrt(own_query) * lax.rsqrt(slope_query_norm + 1e-06))
    mean_key = mean_key * (jnp.sqrt(own_key) * lax.rsqrt(slope_key_norm + 1e-06))
    mean_value = mean_value * (jnp.sqrt(own_value) * lax.rsqrt(slope_value_norm + 1e-06))
    mean_mixed = mean_mixed * (jnp.sqrt(own_mixed) * lax.rsqrt(slope_mixed_norm + 1e-06))
    state_new_query = hold_rate * state_query + (1.0 - hold_rate) * mean_query * mean_query
    next_query = param_query - learn_rate * mean_query * lax.rsqrt(state_new_query + 1e-06)
    state_new_key = hold_rate * state_key + (1.0 - hold_rate) * mean_key * mean_key
    next_key = param_key - learn_rate * mean_key * lax.rsqrt(state_new_key + 1e-06)
    state_new_value = hold_rate * state_value + (1.0 - hold_rate) * mean_value * mean_value
    next_value = param_value - learn_rate * mean_value * lax.rsqrt(state_new_value + 1e-06)
    state_new_mixed = hold_rate * state_mixed + (1.0 - hold_rate) * mean_mixed * mean_mixed
    next_mixed = param_mixed - learn_rate * mean_mixed * lax.rsqrt(state_new_mixed + 1e-06)
    state_new_norm = hold_rate * state_norm + (1.0 - hold_rate) * mean_norm * mean_norm
    next_norm = param_norm - learn_rate * mean_norm * lax.rsqrt(state_new_norm + 1e-06)
    state_new_bias = hold_rate * state_bias + (1.0 - hold_rate) * mean_bias * mean_bias
    next_bias = param_bias - learn_rate * mean_bias * lax.rsqrt(state_new_bias + 1e-06)
    half_query, half_key, half_value, half_mixed, half_norm, half_bias = (
        lax.all_gather(next_query.astype(jnp.bfloat16), "dp", axis=0, tiled=True),
        lax.all_gather(next_key.astype(jnp.bfloat16), "dp", axis=0, tiled=True),
        lax.all_gather(next_value.astype(jnp.bfloat16), "dp", axis=0, tiled=True),
        lax.all_gather(next_mixed.astype(jnp.bfloat16), "dp", axis=1, tiled=True),
        lax.all_gather(next_norm.astype(jnp.bfloat16), "dp", axis=0, tiled=True),
        lax.all_gather(next_bias.astype(jnp.bfloat16), "dp", axis=0, tiled=True),
    )
    return (
        half_query,
        half_key,
        half_value,
        half_mixed,
        half_norm,
        half_bias,
        next_query,
        next_key,
        next_value,
        next_mixed,
        next_norm,
        next_bias,
        state_new_query,
        state_new_key,
        state_new_value,
        state_new_mixed,
        state_new_norm,
        state_new_bias,
    )


MESH = pl.DeviceIdType.MESH
HALVES = 2
LAG = 2
AHEAD = 4
GAIN = 1024.0
ORDER = (0, 3, 1, 2)


def plan_of(mesh):
    n, pair = mesh.shape["dp"], mesh.shape["tp"]
    return n if pair == 2 and n == 4 else None


def encode(x):
    t = x * GAIN
    t = t * t
    t = t * t
    t = t * t
    return jnp.where(x < 0, -t, t).astype(jnp.bfloat16)


def decode(y):
    y = y.astype(jnp.float32)
    fourth = lax.rsqrt(lax.rsqrt(jnp.abs(y)))
    root = fourth * lax.rsqrt(jnp.maximum(fourth, 1e-30)) * (1.0 / GAIN)
    return jnp.where(y < 0, -root, root)


def update(param, state, mean):
    state_new = hold_rate * state + (1.0 - hold_rate) * mean * mean
    return state_new, param - learn_rate * mean * lax.rsqrt(state_new + 1e-06)


def kernel(n, *refs):
    (sq, sk, sv, sm, sn, sb, pq, pk, pv, pm, pn, pb, tq, tk, tv, tm, tn, tb) = refs[:18]
    (hq, hk, hv, hm, hn, hb, xq, xk, xv, xm, xn, xb, nq, nk, nv, nm, nn, nb) = refs[18:36]
    (X, XM, S, RL, RR, G, P_, T_, NX, NS, TOT, ES, ER, HM, VB, VR, NV,
     load_sem, mix_sem, par_sem, rs_send, rl_sem, rr_sem, ag_send, ag_send2, ag_recv,
     e_send, e_recv, v_send, v_recv, out_sem, half_sem) = refs[36:]
    C, _, B, W = X.shape
    H = HALVES
    own = B * H
    mixc = H * ORDER.index(3)
    me = lax.axis_index("dp")
    core = lax.axis_index("tp")
    rate = float(n) ** (-0.5)
    slopes = (sq, sk, sv)

    def rows_of(h, j=0):
        return pl.ds(j * own + h * B, B)

    loads = [[] for _ in range(C)]
    pars = []
    for at, m in enumerate(ORDER):
        for h in range(H):
            c = at * H + h
            if m < 3:
                for j in range(n):
                    loads[c].append(
                        pltpu.make_async_copy(slopes[m].at[0, rows_of(h, j)], X.at[c, j], load_sem.at[c, j])
                    )
                    loads[c][-1].start()
        if m == 3:
            mix = pltpu.make_async_copy(sm.at[0], XM, mix_sem)
            mix.start()
    for at, m in enumerate(ORDER):
        for h in range(H):
            c = at * H + h
            for k, (src, dst) in enumerate((((pq, pk, pv, pm)[m], P_), ((tq, tk, tv, tm)[m], T_))):
                cp = pltpu.make_async_copy(src.at[rows_of(h)], dst.at[c], par_sem.at[k, c])
                cp.start()
                pars.append(cp)

    barrier = pltpu.get_barrier_semaphore()
    for d in range(1, n):
        pl.semaphore_signal(barrier, inc=1, device_id={"dp": lax.rem(me + d, n)}, device_id_type=MESH)
    pl.semaphore_signal(barrier, inc=1, device_id={"tp": 1 - core}, device_id_type=MESH)

    part = sn.shape[1] // n
    for j in range(n):
        VB[j : j + 1, :part] = sn[:, j * part : (j + 1) * part]
        VB[n + j : n + j + 1, :part] = sb[:, j * part : (j + 1) * part]
    for k, r in enumerate((pn, pb, tn, tb)):
        VB[2 * n + k : 2 * n + k + 1, :part] = r[...]
    pl.semaphore_wait(barrier, n)

    def hop(src, dst, ss, rs, to):
        return pltpu.make_async_remote_copy(
            src_ref=src, dst_ref=dst, send_sem=ss, recv_sem=rs, device_id={"dp": to}, device_id_type=MESH
        )

    right, left = jnp.minimum(me + 1, n - 1), jnp.maximum(me - 1, 0)

    def rs_right(c, j):
        return hop(S.at[c, j], RL.at[c, j], rs_send.at[c, j], rl_sem.at[c, j], right)

    def rs_left(c, j):
        return hop(S.at[c, j], RR.at[c, j], rs_send.at[c, j], rr_sem.at[c, j], left)

    def ag_right(c, j):
        return hop(G.at[c, j], G.at[c, j], ag_send.at[c, j], ag_recv.at[c, j], right)

    def ag_left(c, j):
        return hop(G.at[c, j], G.at[c, j], ag_send.at[c, j], ag_recv.at[c, j], left)

    def ag_left_own(c):
        return hop(G.at[c, me], G.at[c, me], ag_send2.at[c], ag_recv.at[c, me], left)

    def vec(d):
        return hop(VB, VR.at[n - d], v_send.at[d], v_recv.at[n - d], lax.rem(me + d, n))

    def pair(c):
        return pltpu.make_async_remote_copy(
            src_ref=ES.at[c], dst_ref=ER.at[c], send_sem=e_send.at[c], recv_sem=e_recv.at[c],
            device_id={"tp": 1 - core}, device_id_type=MESH,
        )

    def first(c):
        @pl.when(me == 0)
        def _():
            for j in range(n - 1, 0, -1):
                S[c, j] = encode(X[c, j])
                rs_right(c, j).start()

        @pl.when(me == n - 1)
        def _():
            for j in range(n - 1):
                S[c, j] = encode(X[c, j])
                rs_left(c, j).start()

    def plus(c):
        for j in range(n - 1, 0, -1):
            @pl.when(jnp.logical_and(me < j, me > 0))
            def _(j=j):
                rs_right(c, j).wait_recv()
                S[c, j] = encode(decode(RL[c, j]) + X[c, j])
                rs_right(c, j).start()

    def minus(c):
        for j in range(n - 1):
            @pl.when(jnp.logical_and(me > j, me < n - 1))
            def _(j=j):
                rs_left(c, j).wait_recv()
                S[c, j] = encode(decode(RR[c, j]) + X[c, j])
                rs_left(c, j).start()

    def gather_sum(c):
        TOT[c] = X[c, me]

        @pl.when(me > 0)
        def _():
            rs_right(c, me).wait_recv()
            TOT[c] = TOT[c] + decode(RL[c, me])

        @pl.when(me < n - 1)
        def _():
            rs_left(c, me).wait_recv()
            TOT[c] = TOT[c] + decode(RR[c, me])

        mean = TOT[c] * rate
        TOT[c] = mean
        p = P_[c]
        lane = lax.broadcasted_iota(jnp.int32, (B, 128), 1)
        ES[c] = jnp.where(
            lane < 64, jnp.sum(p * p, axis=1, keepdims=True), jnp.sum(mean * mean, axis=1, keepdims=True)
        )
        pair(c).start()

    def apply(c):
        pair(c).wait_recv()
        both = ES[c] + ER[c]
        ratio = jnp.sqrt(both[:, :1]) * lax.rsqrt(both[:, 64:65] + 1e-06)
        state_new, nxt = update(P_[c], T_[c], TOT[c] * ratio)
        G[c, me] = nxt.astype(jnp.bfloat16)
        NX[c] = nxt
        NS[c] = state_new

        @pl.when(me < n - 1)
        def _():
            ag_right(c, me).start()

        @pl.when(me > 0)
        def _():
            ag_left_own(c).start()

    def passes(j):
        return jnp.logical_or(
            jnp.logical_and(me > j, me < n - 1), jnp.logical_and(me < j, me > 0)
        )

    def take(c, j):
        ag_right(c, j).wait_recv()

        @pl.when(jnp.logical_and(me > j, me < n - 1))
        def _():
            ag_right(c, j).start()

        @pl.when(jnp.logical_and(me < j, me > 0))
        def _():
            ag_left(c, j).start()

    def mixed_in():
        mix.wait()
        for b in range(XM.shape[1] // 128):
            t = XM[:, b * 128 : b * 128 + 128].T
            for p in range(4):
                r = b * 128 + p * 32
                X[mixc + (r % own) // B, r // own, r % B : r % B + 32] = t[p * 32 : p * 32 + 32]

    for d in range(1, n):
        vec(d).start()
    VR[0] = VB[...]
    for c in range(H):
        for cp in loads[c]:
            cp.wait()
        first(c)
    for c in range(H, C):
        for cp in loads[c]:
            cp.wait()
    mixed_in()

    for c in range(H, AHEAD):
        first(c)
    for cp in pars:
        cp.wait()

    def step(t, carry):
        @pl.when(t < C - AHEAD)
        def _():
            first(t + AHEAD)

        low = me < n // 2
        tp_, tm_ = jnp.where(low, t, t - 1), jnp.where(low, t - 1, t)

        @pl.when(jnp.logical_and(tp_ >= 0, tp_ < C))
        def _():
            plus(tp_)

        @pl.when(jnp.logical_and(tm_ >= 0, tm_ < C))
        def _():
            minus(tm_)

        @pl.when(jnp.logical_and(t >= LAG, t < C + LAG))
        def _():
            gather_sum(t - LAG)

        @pl.when(jnp.logical_and(t >= LAG + 1, t < C + LAG + 1))
        def _():
            apply(t - LAG - 1)

        @pl.when(t >= LAG + 2)
        def _():
            for j in range(1, n - 1):
                @pl.when(passes(j))
                def _(j=j):
                    take(t - LAG - 2, j)

        return carry

    lax.fori_loop(0, C + LAG + 2, step, 0)

    nexts, news = (xq, xk, xv, xm), (nq, nk, nv, nm)
    outs = []
    for at, m in enumerate(ORDER):
        for k, (buf, dsts) in enumerate(((NX, nexts), (NS, news))):
            for h in range(H):
                c = at * H + h
                cp = pltpu.make_async_copy(buf.at[c], dsts[m].at[rows_of(h)], out_sem.at[k, c])
                cp.start()
                outs.append(cp)

    for d in range(1, n):
        vec(d).wait_send()
        vec(n - d).wait_recv()
    total = VR[0, : 2 * n]
    for d in range(1, n):
        total = total + VR[d, : 2 * n]
    NV[0] = total * rate
    for d in range(n):
        at = lax.rem(me + d, n)
        for k in range(2):
            mean = NV[0, pl.ds(k * n + at, 1), :]
            state_new, nxt = update(
                VR[d, 2 * n + k : 2 * n + k + 1], VR[d, 2 * n + 2 + k : 2 * n + 3 + k], mean
            )
            NV[1, pl.ds(k * n + at, 1), :] = nxt
            if d == 0:
                (xn, xb)[k][...] = nxt[:, :part]
                (nn, nb)[k][...] = state_new[:, :part]
    for k, o in enumerate((hn, hb)):
        o[...] = jnp.concatenate(
            [NV[1, k * n + j : k * n + j + 1, :part] for j in range(n)], axis=1
        ).astype(jnp.bfloat16)

    halves = (hq, hk, hv)

    middle = jnp.logical_and(me > 0, me < n - 1)
    near = jnp.where(me < n // 2, 0, n - 1)

    def finish(t):
        if t < C:
            @pl.when(middle)
            def _():
                take(t, near)
        if t >= 1:
            @pl.when(middle)
            def _():
                take(t - 1, n - 1 - near)

            @pl.when(jnp.logical_not(middle))
            def _():
                for j in range(n):
                    @pl.when(me != j)
                    def _(j=j):
                        take(t - 1, j)

    stores = []
    finish(0)
    for at, m in enumerate(ORDER):
        for h in range(H):
            c = at * H + h
            finish(c + 1)
            if m < 3:
                for j in range(n):
                    cp = pltpu.make_async_copy(G.at[c, j], halves[m].at[rows_of(h, j)], half_sem.at[c, j])
                    cp.start()
                    stores.append(cp)
        if m == 3:
            for j in range(n // 2):
                rows = [G[at * H + h, 2 * j + i].astype(jnp.float32) for i in range(2) for h in range(H)]
                HM[:, j * 2 * own : (j + 1) * 2 * own] = jnp.concatenate(rows, axis=0).T.astype(jnp.bfloat16)
            cp = pltpu.make_async_copy(HM, hm, half_sem.at[at * H, 0])
            cp.start()
            stores.append(cp)

    def drain(c, carry):
        for j in range(n):
            @pl.when(me != j)
            def _(j=j):
                rs_right(c, j).wait_send()

            @pl.when(jnp.logical_and(me != j, passes(j)))
            def _(j=j):
                ag_right(c, j).wait_send()

        @pl.when(me < n - 1)
        def _():
            ag_right(c, me).wait_send()

        @pl.when(me > 0)
        def _():
            ag_left_own(c).wait_send()

        pair(c).wait_send()
        return carry

    lax.fori_loop(0, C, drain, 0)
    for cp in outs + stores:
        cp.wait()


def fused(n, *args):
    slopes, params, states = list(args[:6]), list(args[6:12]), list(args[12:])
    own, width = params[0].shape
    H = HALVES
    B = own // H
    if own % (H * 32) or width % 128 or args[3].shape[1:] != (width, n * own) or args[3].shape[2] % 256:
        return shards(*args)
    C = H * 4
    for group in (params, states):
        group[3] = group[3].T
        for i in (4, 5):
            group[i] = group[i].reshape(1, -1)
    any_, vmem = pl.BlockSpec(memory_space=pltpu.HBM), pl.BlockSpec(memory_space=pltpu.VMEM)
    f32, bf16 = jnp.float32, jnp.bfloat16
    specs = [any_] * 4 + [vmem] * 2
    S = jax.ShapeDtypeStruct
    rows = n * own
    shape = (
        [S((rows, width), bf16)] * 3 + [S((width, rows), bf16)] + [S((1, rows), bf16)] * 2
        + ([S((own, width), f32)] * 4 + [S((1, own), f32)] * 2) * 2
    )
    wide = -(-own // 128) * 128
    dma = pltpu.SemaphoreType.DMA
    outs = pl.pallas_call(
        functools.partial(kernel, n),
        out_shape=shape,
        in_specs=specs * 3,
        out_specs=specs * 3,
        scratch_shapes=[
            pltpu.VMEM((C, n, B, width), f32),
            pltpu.VMEM((width, rows), f32),
            pltpu.VMEM((C, n, B, width), bf16),
            pltpu.VMEM((C, n, B, width), bf16),
            pltpu.VMEM((C, n, B, width), bf16),
            pltpu.VMEM((C, n, B, width), bf16),
            pltpu.VMEM((C, B, width), f32),
            pltpu.VMEM((C, B, width), f32),
            pltpu.VMEM((C, B, width), f32),
            pltpu.VMEM((C, B, width), f32),
            pltpu.VMEM((C, B, width), f32),
            pltpu.VMEM((C, B, 128), f32),
            pltpu.VMEM((C, B, 128), f32),
            pltpu.VMEM((width, rows), bf16),
            pltpu.VMEM((16, wide), f32),
            pltpu.VMEM((n, 16, wide), f32),
            pltpu.VMEM((2, 2 * n, wide), f32),
            dma((C, n)), dma, dma((2, C)), dma((C, n)), dma((C, n)), dma((C, n)), dma((C, n)), dma((C,)), dma((C, n)),
            dma((C,)), dma((C,)), dma((n,)), dma((n,)), dma((2, C)), dma((C, n)),
        ],
        compiler_params=pltpu.CompilerParams(
            collective_id=0, has_side_effects=True, vmem_limit_bytes=67043328
        ),
        cost_estimate=pl.CostEstimate(flops=10**7, bytes_accessed=10**7, transcendentals=0),
    )(*slopes, *params, *states)
    outs = list(outs)
    for k in (9, 15):
        outs[k] = outs[k].T
    for k in (4, 5, 10, 11, 16, 17):
        outs[k] = outs[k].reshape(-1)
    return tuple(outs)


def solution(mesh):
    in_specs = (
        P(("trial", "dp"), None, "tp"),
        P(("trial", "dp"), None, "tp"),
        P(("trial", "dp"), None, "tp"),
        P(("trial", "dp"), "tp", None),
        P(("trial", "dp"), None),
        P(("trial", "dp"), None),
        P(("trial", "dp"), "tp"),
        P(("trial", "dp"), "tp"),
        P(("trial", "dp"), "tp"),
        P(("trial", "tp"), "dp"),
        P(("trial", "dp")),
        P(("trial", "dp")),
        P(("trial", "dp"), "tp"),
        P(("trial", "dp"), "tp"),
        P(("trial", "dp"), "tp"),
        P(("trial", "tp"), "dp"),
        P(("trial", "dp")),
        P(("trial", "dp")),
    )
    out_specs = (
        P("trial", "tp"),
        P("trial", "tp"),
        P("trial", "tp"),
        P(("trial", "tp"), None),
        P("trial"),
        P("trial"),
        P(("trial", "dp"), "tp"),
        P(("trial", "dp"), "tp"),
        P(("trial", "dp"), "tp"),
        P(("trial", "tp"), "dp"),
        P(("trial", "dp")),
        P(("trial", "dp")),
        P(("trial", "dp"), "tp"),
        P(("trial", "dp"), "tp"),
        P(("trial", "dp"), "tp"),
        P(("trial", "tp"), "dp"),
        P(("trial", "dp")),
        P(("trial", "dp")),
    )
    plan = plan_of(mesh)
    body = shards if plan is None else functools.partial(fused, plan)
    return jax.shard_map(body, mesh=mesh, in_specs=in_specs, out_specs=out_specs, check_vma=False)
```

```python
import functools

import jax
import jax.numpy as jnp
from jax import lax
from jax.experimental import pallas as pl
from jax.experimental.pallas import tpu as pltpu
from jax.sharding import PartitionSpec as P

learn_rate = 0.02
hold_rate = 0.8


def shards(
    slope_query,
    slope_key,
    slope_value,
    slope_mixed,
    slope_norm,
    slope_bias,
    param_query,
    param_key,
    param_value,
    param_mixed,
    param_norm,
    param_bias,
    state_query,
    state_key,
    state_value,
    state_mixed,
    state_norm,
    state_bias,
):
    mean_query, mean_key, mean_value, mean_mixed = (
        lax.psum_scatter(slope_query[0], "dp", scatter_dimension=0, tiled=True),
        lax.psum_scatter(slope_key[0], "dp", scatter_dimension=0, tiled=True),
        lax.psum_scatter(slope_value[0], "dp", scatter_dimension=0, tiled=True),
        lax.psum_scatter(slope_mixed[0], "dp", scatter_dimension=1, tiled=True),
    )
    whole_norm, whole_bias = lax.psum((slope_norm[0], slope_bias[0]), "dp")
    place = lax.axis_index("dp")
    mean_norm = lax.dynamic_slice_in_dim(
        whole_norm, place * param_norm.shape[0], param_norm.shape[0]
    )
    mean_bias = lax.dynamic_slice_in_dim(
        whole_bias, place * param_bias.shape[0], param_bias.shape[0]
    )
    mean_rate = lax.axis_size("dp") ** (-0.5)
    mean_query = mean_query * mean_rate
    mean_key = mean_key * mean_rate
    mean_value = mean_value * mean_rate
    mean_mixed = mean_mixed * mean_rate
    mean_norm = mean_norm * mean_rate
    mean_bias = mean_bias * mean_rate
    (
        own_query,
        own_key,
        own_value,
        own_mixed,
        slope_query_norm,
        slope_key_norm,
        slope_value_norm,
        slope_mixed_norm,
    ) = lax.psum(
        (
            jnp.sum(param_query * param_query, axis=1, keepdims=True),
            jnp.sum(param_key * param_key, axis=1, keepdims=True),
            jnp.sum(param_value * param_value, axis=1, keepdims=True),
            jnp.sum(param_mixed * param_mixed, axis=0, keepdims=True),
            jnp.sum(mean_query * mean_query, axis=1, keepdims=True),
            jnp.sum(mean_key * mean_key, axis=1, keepdims=True),
            jnp.sum(mean_value * mean_value, axis=1, keepdims=True),
            jnp.sum(mean_mixed * mean_mixed, axis=0, keepdims=True),
        ),
        "tp",
    )
    mean_query = mean_query * (jnp.sqrt(own_query) * lax.rsqrt(slope_query_norm + 1e-06))
    mean_key = mean_key * (jnp.sqrt(own_key) * lax.rsqrt(slope_key_norm + 1e-06))
    mean_value = mean_value * (jnp.sqrt(own_value) * lax.rsqrt(slope_value_norm + 1e-06))
    mean_mixed = mean_mixed * (jnp.sqrt(own_mixed) * lax.rsqrt(slope_mixed_norm + 1e-06))
    state_new_query = hold_rate * state_query + (1.0 - hold_rate) * mean_query * mean_query
    next_query = param_query - learn_rate * mean_query * lax.rsqrt(state_new_query + 1e-06)
    state_new_key = hold_rate * state_key + (1.0 - hold_rate) * mean_key * mean_key
    next_key = param_key - learn_rate * mean_key * lax.rsqrt(state_new_key + 1e-06)
    state_new_value = hold_rate * state_value + (1.0 - hold_rate) * mean_value * mean_value
    next_value = param_value - learn_rate * mean_value * lax.rsqrt(state_new_value + 1e-06)
    state_new_mixed = hold_rate * state_mixed + (1.0 - hold_rate) * mean_mixed * mean_mixed
    next_mixed = param_mixed - learn_rate * mean_mixed * lax.rsqrt(state_new_mixed + 1e-06)
    state_new_norm = hold_rate * state_norm + (1.0 - hold_rate) * mean_norm * mean_norm
    next_norm = param_norm - learn_rate * mean_norm * lax.rsqrt(state_new_norm + 1e-06)
    state_new_bias = hold_rate * state_bias + (1.0 - hold_rate) * mean_bias * mean_bias
    next_bias = param_bias - learn_rate * mean_bias * lax.rsqrt(state_new_bias + 1e-06)
    half_query, half_key, half_value, half_mixed, half_norm, half_bias = (
        lax.all_gather(next_query.astype(jnp.bfloat16), "dp", axis=0, tiled=True),
        lax.all_gather(next_key.astype(jnp.bfloat16), "dp", axis=0, tiled=True),
        lax.all_gather(next_value.astype(jnp.bfloat16), "dp", axis=0, tiled=True),
        lax.all_gather(next_mixed.astype(jnp.bfloat16), "dp", axis=1, tiled=True),
        lax.all_gather(next_norm.astype(jnp.bfloat16), "dp", axis=0, tiled=True),
        lax.all_gather(next_bias.astype(jnp.bfloat16), "dp", axis=0, tiled=True),
    )
    return (
        half_query,
        half_key,
        half_value,
        half_mixed,
        half_norm,
        half_bias,
        next_query,
        next_key,
        next_value,
        next_mixed,
        next_norm,
        next_bias,
        state_new_query,
        state_new_key,
        state_new_value,
        state_new_mixed,
        state_new_norm,
        state_new_bias,
    )


MESH = pl.DeviceIdType.MESH
HALVES = 2
LAG = 2
AHEAD = 4
GAIN = 1024.0
ORDER = (0, 3, 1, 2)


def plan_of(mesh):
    n, pair = mesh.shape["dp"], mesh.shape["tp"]
    return n if pair == 2 and n == 4 else None


def encode(x):
    t = x * GAIN
    t = t * t
    t = t * t
    t = t * t
    return jnp.where(x < 0, -t, t).astype(jnp.bfloat16)


def decode(y):
    y = y.astype(jnp.float32)
    fourth = lax.rsqrt(lax.rsqrt(jnp.abs(y)))
    root = fourth * lax.rsqrt(jnp.maximum(fourth, 1e-30)) * (1.0 / GAIN)
    return jnp.where(y < 0, -root, root)


def update(param, state, mean):
    state_new = hold_rate * state + (1.0 - hold_rate) * mean * mean
    return state_new, param - learn_rate * mean * lax.rsqrt(state_new + 1e-06)


def kernel(n, *refs):
    (sq, sk, sv, sm, sn, sb, pq, pk, pv, pm, pn, pb, tq, tk, tv, tm, tn, tb) = refs[:18]
    (hq, hk, hv, hm, hn, hb, xq, xk, xv, xm, xn, xb, nq, nk, nv, nm, nn, nb) = refs[18:36]
    (X, XM, S, RL, RR, G, P_, T_, NX, NS, TOT, ES, ER, HM, VB, VR, NV,
     load_sem, mix_sem, par_sem, rs_send, rl_sem, rr_sem, ag_send, ag_send2, ag_recv,
     e_send, e_recv, v_send, v_recv, out_sem, half_sem) = refs[36:]
    C, _, B, W = X.shape
    H = HALVES
    own = B * H
    mixc = H * ORDER.index(3)
    me = lax.axis_index("dp")
    core = lax.axis_index("tp")
    rate = float(n) ** (-0.5)
    slopes = (sq, sk, sv)

    def rows_of(h, j=0):
        return pl.ds(j * own + h * B, B)

    loads = [[] for _ in range(C)]
    pars = []
    for at, m in enumerate(ORDER):
        for h in range(H):
            c = at * H + h
            if m < 3:
                for j in range(n):
                    loads[c].append(
                        pltpu.make_async_copy(slopes[m].at[0, rows_of(h, j)], X.at[c, j], load_sem.at[c, j])
                    )
                    loads[c][-1].start()
        if m == 3:
            mix = pltpu.make_async_copy(sm.at[0], XM, mix_sem)
            mix.start()
    for at, m in enumerate(ORDER):
        for h in range(H):
            c = at * H + h
            for k, (src, dst) in enumerate((((pq, pk, pv, pm)[m], P_), ((tq, tk, tv, tm)[m], T_))):
                cp = pltpu.make_async_copy(src.at[rows_of(h)], dst.at[c], par_sem.at[k, c])
                cp.start()
                pars.append(cp)

    barrier = pltpu.get_barrier_semaphore()
    for d in range(1, n):
        pl.semaphore_signal(barrier, inc=1, device_id={"dp": lax.rem(me + d, n)}, device_id_type=MESH)
    pl.semaphore_signal(barrier, inc=1, device_id={"tp": 1 - core}, device_id_type=MESH)

    part = sn.shape[1] // n
    for j in range(n):
        VB[j : j + 1, :part] = sn[:, j * part : (j + 1) * part]
        VB[n + j : n + j + 1, :part] = sb[:, j * part : (j + 1) * part]
    for k, r in enumerate((pn, pb, tn, tb)):
        VB[2 * n + k : 2 * n + k + 1, :part] = r[...]
    pl.semaphore_wait(barrier, n)

    def hop(src, dst, ss, rs, to):
        return pltpu.make_async_remote_copy(
            src_ref=src, dst_ref=dst, send_sem=ss, recv_sem=rs, device_id={"dp": to}, device_id_type=MESH
        )

    right, left = jnp.minimum(me + 1, n - 1), jnp.maximum(me - 1, 0)

    def rs_right(c, j):
        return hop(S.at[c, j], RL.at[c, j], rs_send.at[c, j], rl_sem.at[c, j], right)

    def rs_left(c, j):
        return hop(S.at[c, j], RR.at[c, j], rs_send.at[c, j], rr_sem.at[c, j], left)

    def ag_right(c, j):
        return hop(G.at[c, j], G.at[c, j], ag_send.at[c, j], ag_recv.at[c, j], right)

    def ag_left(c, j):
        return hop(G.at[c, j], G.at[c, j], ag_send.at[c, j], ag_recv.at[c, j], left)

    def ag_left_own(c):
        return hop(G.at[c, me], G.at[c, me], ag_send2.at[c], ag_recv.at[c, me], left)

    def vec(d):
        return hop(VB, VR.at[n - d], v_send.at[d], v_recv.at[n - d], lax.rem(me + d, n))

    def pair(c):
        return pltpu.make_async_remote_copy(
            src_ref=ES.at[c], dst_ref=ER.at[c], send_sem=e_send.at[c], recv_sem=e_recv.at[c],
            device_id={"tp": 1 - core}, device_id_type=MESH,
        )

    def first(c):
        @pl.when(me == 0)
        def _():
            for j in range(n - 1, 0, -1):
                S[c, j] = encode(X[c, j])
                rs_right(c, j).start()

        @pl.when(me == n - 1)
        def _():
            for j in range(n - 1):
                S[c, j] = encode(X[c, j])
                rs_left(c, j).start()

    def plus(c):
        for j in range(n - 1, 0, -1):
            @pl.when(jnp.logical_and(me < j, me > 0))
            def _(j=j):
                rs_right(c, j).wait_recv()
                S[c, j] = encode(decode(RL[c, j]) + X[c, j])
                rs_right(c, j).start()

    def minus(c):
        for j in range(n - 1):
            @pl.when(jnp.logical_and(me > j, me < n - 1))
            def _(j=j):
                rs_left(c, j).wait_recv()
                S[c, j] = encode(decode(RR[c, j]) + X[c, j])
                rs_left(c, j).start()

    def gather_sum(c):
        TOT[c] = X[c, me]

        @pl.when(me > 0)
        def _():
            rs_right(c, me).wait_recv()
            TOT[c] = TOT[c] + decode(RL[c, me])

        @pl.when(me < n - 1)
        def _():
            rs_left(c, me).wait_recv()
            TOT[c] = TOT[c] + decode(RR[c, me])

        mean = TOT[c] * rate
        TOT[c] = mean
        p = P_[c]
        lane = lax.broadcasted_iota(jnp.int32, (B, 128), 1)
        ES[c] = jnp.where(
            lane < 64, jnp.sum(p * p, axis=1, keepdims=True), jnp.sum(mean * mean, axis=1, keepdims=True)
        )
        pair(c).start()

    def apply(c):
        pair(c).wait_recv()
        both = ES[c] + ER[c]
        ratio = jnp.sqrt(both[:, :1]) * lax.rsqrt(both[:, 64:65] + 1e-06)
        state_new, nxt = update(P_[c], T_[c], TOT[c] * ratio)
        G[c, me] = nxt.astype(jnp.bfloat16)
        NX[c] = nxt
        NS[c] = state_new

        @pl.when(me < n - 1)
        def _():
            ag_right(c, me).start()

        @pl.when(me > 0)
        def _():
            ag_left_own(c).start()

    def passes(j):
        return jnp.logical_or(
            jnp.logical_and(me > j, me < n - 1), jnp.logical_and(me < j, me > 0)
        )

    def take(c, j):
        ag_right(c, j).wait_recv()

        @pl.when(jnp.logical_and(me > j, me < n - 1))
        def _():
            ag_right(c, j).start()

        @pl.when(jnp.logical_and(me < j, me > 0))
        def _():
            ag_left(c, j).start()

    def mixed_in():
        mix.wait()
        for b in range(XM.shape[1] // 128):
            t = XM[:, b * 128 : b * 128 + 128].T
            for p in range(4):
                r = b * 128 + p * 32
                X[mixc + (r % own) // B, r // own, r % B : r % B + 32] = t[p * 32 : p * 32 + 32]

    for d in range(1, n):
        vec(d).start()
    VR[0] = VB[...]
    for c in range(H):
        for cp in loads[c]:
            cp.wait()
        first(c)
    for c in range(H, C):
        for cp in loads[c]:
            cp.wait()
    mixed_in()

    for c in range(H, AHEAD):
        first(c)
    for cp in pars:
        cp.wait()

    def step(t, carry):
        @pl.when(t < C - AHEAD)
        def _():
            first(t + AHEAD)

        low = me < n // 2
        tp_, tm_ = jnp.where(low, t, t - 1), jnp.where(low, t - 1, t)

        @pl.when(jnp.logical_and(tp_ >= 0, tp_ < C))
        def _():
            plus(tp_)

        @pl.when(jnp.logical_and(tm_ >= 0, tm_ < C))
        def _():
            minus(tm_)

        @pl.when(jnp.logical_and(t >= LAG, t < C + LAG))
        def _():
            gather_sum(t - LAG)

        @pl.when(jnp.logical_and(t >= LAG + 1, t < C + LAG + 1))
        def _():
            apply(t - LAG - 1)

        @pl.when(t >= LAG + 2)
        def _():
            for j in range(1, n - 1):
                @pl.when(passes(j))
                def _(j=j):
                    take(t - LAG - 2, j)

        return carry

    lax.fori_loop(0, C + LAG + 2, step, 0)

    nexts, news = (xq, xk, xv, xm), (nq, nk, nv, nm)
    outs = []
    for at, m in enumerate(ORDER):
        for k, (buf, dsts) in enumerate(((NX, nexts), (NS, news))):
            for h in range(H):
                c = at * H + h
                cp = pltpu.make_async_copy(buf.at[c], dsts[m].at[rows_of(h)], out_sem.at[k, c])
                cp.start()
                outs.append(cp)

    for d in range(1, n):
        vec(d).wait_send()
        vec(n - d).wait_recv()
    total = VR[0, : 2 * n]
    for d in range(1, n):
        total = total + VR[d, : 2 * n]
    NV[0] = total * rate
    for d in range(n):
        at = lax.rem(me + d, n)
        for k in range(2):
            mean = NV[0, pl.ds(k * n + at, 1), :]
            state_new, nxt = update(
                VR[d, 2 * n + k : 2 * n + k + 1], VR[d, 2 * n + 2 + k : 2 * n + 3 + k], mean
            )
            NV[1, pl.ds(k * n + at, 1), :] = nxt
            if d == 0:
                (xn, xb)[k][...] = nxt[:, :part]
                (nn, nb)[k][...] = state_new[:, :part]
    for k, o in enumerate((hn, hb)):
        o[...] = jnp.concatenate(
            [NV[1, k * n + j : k * n + j + 1, :part] for j in range(n)], axis=1
        ).astype(jnp.bfloat16)

    halves = (hq, hk, hv)

    middle = jnp.logical_and(me > 0, me < n - 1)
    near = jnp.where(me < n // 2, 0, n - 1)

    def finish(t):
        if t < C:
            @pl.when(middle)
            def _():
                take(t, near)
        if t >= 1:
            @pl.when(middle)
            def _():
                take(t - 1, n - 1 - near)

            @pl.when(jnp.logical_not(middle))
            def _():
                for j in range(n):
                    @pl.when(me != j)
                    def _(j=j):
                        take(t - 1, j)

    stores = []
    finish(0)
    for at, m in enumerate(ORDER):
        for h in range(H):
            c = at * H + h
            finish(c + 1)
            if m < 3:
                for j in range(n):
                    cp = pltpu.make_async_copy(G.at[c, j], halves[m].at[rows_of(h, j)], half_sem.at[c, j])
                    cp.start()
                    stores.append(cp)
        if m == 3:
            for j in range(n // 2):
                rows = [G[at * H + h, 2 * j + i].astype(jnp.float32) for i in range(2) for h in range(H)]
                HM[:, j * 2 * own : (j + 1) * 2 * own] = jnp.concatenate(rows, axis=0).T.astype(jnp.bfloat16)
            cp = pltpu.make_async_copy(HM, hm, half_sem.at[at * H, 0])
            cp.start()
            stores.append(cp)

    def drain(c, carry):
        for j in range(n):
            @pl.when(me != j)
            def _(j=j):
                rs_right(c, j).wait_send()

            @pl.when(jnp.logical_and(me != j, passes(j)))
            def _(j=j):
                ag_right(c, j).wait_send()

        @pl.when(me < n - 1)
        def _():
            ag_right(c, me).wait_send()

        @pl.when(me > 0)
        def _():
            ag_left_own(c).wait_send()

        pair(c).wait_send()
        return carry

    lax.fori_loop(0, C, drain, 0)
    for cp in outs + stores:
        cp.wait()


def settle(count, *refs):
    src, dst, mid = refs[:count], refs[count : 2 * count], refs[2 * count : 3 * count]
    got, put = refs[3 * count :]
    ins = [pltpu.make_async_copy(src[i], mid[i], got.at[i]) for i in range(count)]
    outs = [pltpu.make_async_copy(mid[i], dst[i], put.at[i]) for i in range(count)]
    for cp in ins:
        cp.start()
    for a, b in zip(ins, outs):
        a.wait()
        b.start()
    for cp in outs:
        cp.wait()


def fused(n, *args):
    slopes, params, states = list(args[:6]), list(args[6:12]), list(args[12:])
    own, width = params[0].shape
    H = HALVES
    B = own // H
    if own % (H * 32) or width % 128 or args[3].shape[1:] != (width, n * own) or args[3].shape[2] % 256:
        return shards(*args)
    C = H * 4
    for group in (params, states):
        group[3] = group[3].T
        for i in (4, 5):
            group[i] = group[i].reshape(1, -1)
    any_, vmem = pl.BlockSpec(memory_space=pltpu.HBM), pl.BlockSpec(memory_space=pltpu.VMEM)
    f32, bf16 = jnp.float32, jnp.bfloat16
    specs = [any_] * 4 + [vmem] * 2
    S = jax.ShapeDtypeStruct
    rows = n * own
    shape = (
        [S((rows, width), bf16)] * 3 + [S((width, rows), bf16)] + [S((1, rows), bf16)] * 2
        + ([S((own, width), f32)] * 4 + [S((1, own), f32)] * 2) * 2
    )
    wide = -(-own // 128) * 128
    dma = pltpu.SemaphoreType.DMA
    outs = pl.pallas_call(
        functools.partial(kernel, n),
        out_shape=shape,
        in_specs=specs * 3,
        out_specs=specs * 3,
        scratch_shapes=[
            pltpu.VMEM((C, n, B, width), f32),
            pltpu.VMEM((width, rows), f32),
            pltpu.VMEM((C, n, B, width), bf16),
            pltpu.VMEM((C, n, B, width), bf16),
            pltpu.VMEM((C, n, B, width), bf16),
            pltpu.VMEM((C, n, B, width), bf16),
            pltpu.VMEM((C, B, width), f32),
            pltpu.VMEM((C, B, width), f32),
            pltpu.VMEM((C, B, width), f32),
            pltpu.VMEM((C, B, width), f32),
            pltpu.VMEM((C, B, width), f32),
            pltpu.VMEM((C, B, 128), f32),
            pltpu.VMEM((C, B, 128), f32),
            pltpu.VMEM((width, rows), bf16),
            pltpu.VMEM((16, wide), f32),
            pltpu.VMEM((n, 16, wide), f32),
            pltpu.VMEM((2, 2 * n, wide), f32),
            dma((C, n)), dma, dma((2, C)), dma((C, n)), dma((C, n)), dma((C, n)), dma((C, n)), dma((C,)), dma((C, n)),
            dma((C,)), dma((C,)), dma((n,)), dma((n,)), dma((2, C)), dma((C, n)),
        ],
        compiler_params=pltpu.CompilerParams(
            collective_id=0, has_side_effects=True, vmem_limit_bytes=67043328
        ),
        cost_estimate=pl.CostEstimate(flops=10**7, bytes_accessed=10**7, transcendentals=0),
    )(*slopes, *params, *states)
    count = len(shape)
    outs = list(
        pl.pallas_call(
            functools.partial(settle, count),
            out_shape=shape,
            in_specs=[any_] * count,
            out_specs=[any_] * count,
            scratch_shapes=[pltpu.VMEM(s.shape, s.dtype) for s in shape] + [dma((count,)), dma((count,))],
            compiler_params=pltpu.CompilerParams(vmem_limit_bytes=67043328),
            cost_estimate=pl.CostEstimate(flops=10**6, bytes_accessed=10**7, transcendentals=0),
        )(*outs)
    )
    for k in (9, 15):
        outs[k] = outs[k].T
    for k in (4, 5, 10, 11, 16, 17):
        outs[k] = outs[k].reshape(-1)
    return tuple(outs)


def solution(mesh):
    in_specs = (
        P(("trial", "dp"), None, "tp"),
        P(("trial", "dp"), None, "tp"),
        P(("trial", "dp"), None, "tp"),
        P(("trial", "dp"), "tp", None),
        P(("trial", "dp"), None),
        P(("trial", "dp"), None),
        P(("trial", "dp"), "tp"),
        P(("trial", "dp"), "tp"),
        P(("trial", "dp"), "tp"),
        P(("trial", "tp"), "dp"),
        P(("trial", "dp")),
        P(("trial", "dp")),
        P(("trial", "dp"), "tp"),
        P(("trial", "dp"), "tp"),
        P(("trial", "dp"), "tp"),
        P(("trial", "tp"), "dp"),
        P(("trial", "dp")),
        P(("trial", "dp")),
    )
    out_specs = (
        P("trial", "tp"),
        P("trial", "tp"),
        P("trial", "tp"),
        P(("trial", "tp"), None),
        P("trial"),
        P("trial"),
        P(("trial", "dp"), "tp"),
        P(("trial", "dp"), "tp"),
        P(("trial", "dp"), "tp"),
        P(("trial", "tp"), "dp"),
        P(("trial", "dp")),
        P(("trial", "dp")),
        P(("trial", "dp"), "tp"),
        P(("trial", "dp"), "tp"),
        P(("trial", "dp"), "tp"),
        P(("trial", "tp"), "dp"),
        P(("trial", "dp")),
        P(("trial", "dp")),
    )
    plan = plan_of(mesh)
    body = shards if plan is None else functools.partial(fused, plan)
    return jax.shard_map(body, mesh=mesh, in_specs=in_specs, out_specs=out_specs, check_vma=False)
```
